32 devices in a mesh: row: 8 (over z, core), col: 4 (over y, x).
Axes of the slice: x: 2, y: 2, z: 4, core: 2. Of those that a mesh axis runs over, the one named last changes fastest.
Arguments:
- sky_image: bfloat16 [2, 16384, 16384], P(None, 'row', 'col'), may hold values from -6 to 6
- facet_rows: int32 [32], replicated, may hold values from 512 to 15872
- facet_offsets: int32 [32], replicated, may hold values from 0 to 511
- facet_owner: int32 [32], replicated, may hold values from 0 to 31, each once
Outputs:
- facets: bfloat16 [32, 2, 1024, 1024], P(('row', 'col'))
The draws below stay inside these ranges and needn't reach their ends.
Inputs may be any that keep to these rules, and one draw needn't show every extreme that they name: `facet_owner`: the entries are distinct, so every device owns exactly one facet.
All inputs are finite; a program needn't handle non-finite values.
Results may differ from the reference program's by a relative error of at most 0.0095.
Values may be sent and summed in bfloat16 or wider, within the bound.
A program may use at most 320 MiB of HBM per device.

```python
import math
import jax
import jax.numpy as jnp
from jax import lax

N = 16384
FS = 1024
SPLIT = 128
BLOCKS = 32
STRIP = 512
LEAD = 128
FACETS = 32


def plant(drawn, own_key, low, high):
    longest = drawn.shape.index(max(drawn.shape))
    spots = []
    for shift in (0, 1):
        where = [jax.random.randint(jax.random.fold_in(own_key, axis), (), 0, length) for axis, length in enumerate(drawn.shape)]
        where[longest] = (where[longest] + shift) % drawn.shape[longest]
        spots.append(tuple(where))
    return drawn.at[spots[0]].set(low).at[spots[1]].set(high)


def level_of(key, dims, split, low, largest):
    loudness = 1.0
    for position, parts in split:
        draws = jax.random.uniform(jax.random.fold_in(jax.random.fold_in(key, 6), position), (parts,), jnp.float32, low / len(split), largest / len(split))
        loudness = loudness * jnp.repeat(jnp.exp(draws), dims[position] // parts).reshape((-1,) + (1,) * (len(dims) - 1 - position))
    return loudness


def centred(rng, dims, scale, most, shards=(), kind=jnp.bfloat16):
    result = scale * jax.random.normal(rng, dims, jnp.float32)
    if shards:
        result = result * level_of(rng, dims, shards, -0.22, 0.18)
    return jnp.clip(result, -most, most).astype(kind)


def setup_inputs(seed: int = 0) -> dict:
    streams_of = jax.random.split(jax.random.key(seed), 5)
    sky_image = centred(streams_of[0], (2, N, N), 1.0, 6.0, ((1, 8), (2, 4)))
    facet_rows = plant(jax.random.randint(streams_of[1], (FACETS,), FS // 2, N - FS // 2 + 1), jax.random.fold_in(streams_of[1], 1), FS // 2, (N - FS // 2 + 1) - 1).astype(jnp.int32)
    facet_offsets = plant(jax.random.randint(streams_of[2], (FACETS,), 0, STRIP), jax.random.fold_in(streams_of[2], 1), 0, STRIP - 1).astype(jnp.int32)
    facet_owner = jax.random.permutation(streams_of[3], BLOCKS).astype(jnp.int32)
    return dict(sky_image=sky_image, facet_rows=facet_rows, facet_offsets=facet_offsets, facet_owner=facet_owner)


def dft_table(length):
    positions = jnp.arange(length, dtype=jnp.int32)
    turn_count = positions[:, None] * positions[None, :] % length
    angles = turn_count.astype(jnp.float32) * (-2.0 * math.pi / length)
    factor = 1.0 / math.sqrt(length)
    return ((jnp.cos(angles) * factor).astype(jnp.bfloat16), (jnp.sin(angles) * factor).astype(jnp.bfloat16))

def twiddle_table(first_len, second_len, total):
    left_index = jnp.arange(first_len, dtype=jnp.int32)[:, None]
    right_index = jnp.arange(second_len, dtype=jnp.int32)[None, :]
    angles = (left_index * right_index % total).astype(jnp.float32) * (-2.0 * math.pi / total)
    return (jnp.cos(angles), jnp.sin(angles))

def complex_mix(formula, tables, values):
    tab_re = tables[0].astype(jnp.float32)
    tab_im = tables[1].astype(jnp.float32)
    val_re = values[0].astype(jnp.float32)
    val_im = values[1].astype(jnp.float32)
    re_part = jnp.einsum(formula, tab_re, val_re) - jnp.einsum(formula, tab_im, val_im)
    im_part = jnp.einsum(formula, tab_re, val_im) + jnp.einsum(formula, tab_im, val_re)
    return (re_part, im_part)

def rotate(pair, twiddle):
    return (pair[0] * twiddle[0] - pair[1] * twiddle[1], pair[0] * twiddle[1] + pair[1] * twiddle[0])

def as_stored(pair):
    return jnp.stack((pair[0].astype(jnp.bfloat16), pair[1].astype(jnp.bfloat16)))

def rows_pass(strip_rows):
    blocks = strip_rows.reshape(2, STRIP, LEAD, SPLIT)
    mixed_pair = complex_mix('pa,rab->rpb', dft_table(LEAD), (blocks[0], blocks[1]))
    section_one = as_stored(rotate(mixed_pair, twiddle_table(LEAD, SPLIT, N)))
    mixed_pair = complex_mix('qb,rpb->rqp', dft_table(SPLIT), (section_one[0], section_one[1]))
    return as_stored(mixed_pair).reshape(2, STRIP, N)

def columns_pass(strip_cols):
    grouped = strip_cols.reshape(2, BLOCKS, STRIP, STRIP)
    mixed_pair = complex_mix('pg,gic->pic', dft_table(BLOCKS), (grouped[0], grouped[1]))
    twiddle = twiddle_table(BLOCKS, STRIP, N)
    section_two = as_stored(rotate(mixed_pair, (twiddle[0][:, :, None], twiddle[1][:, :, None])))
    mixed_pair = complex_mix('qi,pic->qpc', dft_table(STRIP), (section_two[0], section_two[1]))
    return as_stored(mixed_pair).reshape(2, N, STRIP)

def reference(sky_image, facet_rows, facet_offsets, facet_owner):
    row_blocks = jnp.moveaxis(sky_image.reshape(2, BLOCKS, STRIP, N), 1, 0)
    done_blocks = lax.map(rows_pass, row_blocks)
    rows_done = jnp.moveaxis(done_blocks, 0, 1).reshape(2, N, N)
    col_blocks = jnp.moveaxis(rows_done.reshape(2, N, BLOCKS, STRIP), 2, 0)
    grid_blocks = lax.map(columns_pass, col_blocks)
    grid_full = jnp.moveaxis(grid_blocks, 0, 2).reshape(2, N, N)
    device_ids = jnp.arange(BLOCKS, dtype=jnp.int32)
    matches = (facet_owner[None, :] == device_ids[:, None]).astype(jnp.int32)
    owned_count = lax.optimization_barrier(jnp.sum(matches, axis=1))
    centre_row = jnp.where(owned_count > 0, lax.optimization_barrier(jnp.sum(matches * facet_rows[None, :], axis=1)), FS // 2)
    centre_col = lax.optimization_barrier(jnp.sum(matches * facet_offsets[None, :], axis=1))
    taper_axis = 0.25 + 0.75 * jnp.sin(math.pi * (jnp.arange(FS, dtype=jnp.float32) + 0.5) / FS)

    def cut_facet(packed):
        device, row_at, col_at, owned = packed
        start_row = (row_at - FS // 2).astype(jnp.int32)
        band_rows = lax.dynamic_slice_in_dim(grid_full, start_row, FS, 1)
        col_index = ((device * STRIP + col_at - FS // 2 + jnp.arange(FS, dtype=jnp.int32)) % N).astype(jnp.int32)
        tile = jnp.take(band_rows, col_index, axis=2)
        weight = taper_axis[:, None] * taper_axis[None, :] * owned.astype(jnp.float32)
        return (tile.astype(jnp.float32) * weight).astype(jnp.bfloat16)
    return lax.map(cut_facet, (device_ids, centre_row, centre_col, owned_count))
```

```python
import math

import jax
import jax.numpy as jnp
from jax import lax
from jax.sharding import PartitionSpec as P


N = 16384
FS = 1024
SPLIT = 128
PARTS = (1, 2, 2, 2, 1)
AHEAD = 2


def shifted(block, axis, distance):
    devices = range(lax.axis_size(axis))
    route = [((i - distance) % len(devices), i) for i in devices]
    return lax.ppermute(block, axis, route)


def dft_table(length):
    positions = jnp.arange(length, dtype=jnp.int32)
    turn_count = positions[:, None] * positions[None, :] % length
    angles = turn_count.astype(jnp.float32) * (-2.0 * math.pi / length)
    factor = 1.0 / math.sqrt(length)
    return (
        (jnp.cos(angles) * factor).astype(jnp.bfloat16),
        (jnp.sin(angles) * factor).astype(jnp.bfloat16),
    )


def twiddle_table(first_len, second_len, total):
    left_index = jnp.arange(first_len, dtype=jnp.int32)[:, None]
    right_index = jnp.arange(second_len, dtype=jnp.int32)[None, :]
    angles = (left_index * right_index % total).astype(jnp.float32) * (-2.0 * math.pi / total)
    return (jnp.cos(angles), jnp.sin(angles))


def paired_table(length):
    re_table, im_table = dft_table(length)
    return jnp.stack(
        (jnp.stack((re_table, -im_table), axis=1), jnp.stack((im_table, re_table), axis=1))
    )


def mix(formula, table, values):
    return jnp.einsum(formula, table, values, preferred_element_type=jnp.float32)


def rotate(pair, twiddle):
    return (
        pair[0] * twiddle[0] - pair[1] * twiddle[1],
        pair[0] * twiddle[1] + pair[1] * twiddle[0],
    )


def rows_pass(parts, order, devices):
    sources, _, row_count, width = parts.shape
    lead_len = N // SPLIT
    blocks = parts.reshape(sources, 2, row_count, width // SPLIT, SPLIT)
    blocks = blocks.transpose(2, 1, 0, 3, 4).reshape(row_count, 2 * lead_len, SPLIT)
    first = paired_table(lead_len).reshape(2 * lead_len, 2, sources, -1)
    first = jnp.take(first, order, axis=2).reshape(2 * lead_len, -1)
    mixed = mix("ka,rab->rkb", first, blocks)
    turned = rotate((mixed[:, :lead_len], mixed[:, lead_len:]), twiddle_table(lead_len, SPLIT, N))
    section_one = jnp.concatenate([part.astype(jnp.bfloat16) for part in turned], axis=2)
    table = paired_table(SPLIT).transpose(1, 0, 2, 3).reshape(2 * SPLIT, 2 * SPLIT)
    done = mix("kb,rpb->rkp", table, section_one).astype(jnp.bfloat16)
    return done.reshape(row_count, devices, -1, lead_len).transpose(1, 0, 2, 3)


def strip_table(devices, spans):
    pairs = paired_table(devices)
    eye = jnp.eye(spans, dtype=jnp.bfloat16)
    full = pairs.transpose(0, 1, 3, 2)[:, None, :, :, None, :] * eye[None, :, None, None, :, None]
    return full.reshape(2 * spans * devices, devices, spans * 2)


def shards(sky_image, facet_rows, facet_offsets, facet_owner):
    row_devices = lax.axis_size("row")
    col_devices = lax.axis_size("col")
    devices = row_devices * col_devices
    strip_len = sky_image.shape[1] // col_devices
    sizes = [part * strip_len // sum(PARTS) for part in PARTS]
    starts = [sum(sizes[:place]) for place in range(len(sizes))]
    my_index = lax.axis_index(("row", "col"))
    device_ids = jnp.arange(devices, dtype=jnp.int32)
    matches = (facet_owner[None, :] == device_ids[:, None]).astype(jnp.int32)
    owned_count = jnp.sum(matches, axis=1)
    centre_row = jnp.where(owned_count > 0, jnp.sum(matches * facet_rows[None, :], axis=1), FS // 2)
    centre_col = jnp.sum(matches * facet_offsets[None, :], axis=1)

    lead_len = N // SPLIT
    spans = SPLIT // devices
    col_width = spans * lead_len
    reach_blocks = FS // (2 * col_width)
    distances = range(reach_blocks, -reach_blocks - 1, -1)
    steps = FS // devices + 1
    full_table = paired_table(strip_len).reshape(2, strip_len, 2, strip_len)
    tables, heads = [], []
    for distance in distances:
        start_row = centre_row[(my_index + distance) % devices] - FS // 2
        first_step = jnp.clip(start_row // devices, 0, strip_len - steps)
        tables.append(lax.dynamic_slice_in_dim(full_table, first_step, steps, 1))
        heads.append(start_row - first_step * devices)
    sides = [place for place, distance in enumerate(distances) if distance != 0]
    groups = [sides, [len(sides) // 2]]
    group_tables = [
        jnp.concatenate([tables[place] for place in group]).reshape(-1, 2, strip_len)
        for group in groups
    ]
    full_twiddle = twiddle_table(devices, strip_len, N)

    my_col = lax.axis_index("col")
    order = my_col ^ jnp.arange(col_devices, dtype=jnp.int32)
    image = sky_image.reshape(2, col_devices, strip_len, -1)

    def fetch(place, after):
        here = my_col
        if after is not None:
            here = lax.optimization_barrier((here, after))[0]
        pieces = []
        for hop in range(col_devices):
            sent = lax.dynamic_slice(
                image, (0, here ^ hop, starts[place], 0), (2, 1, sizes[place], image.shape[3])
            )[:, 0]
            if hop:
                sent = lax.ppermute(sent, "col", [(i, i ^ hop) for i in range(col_devices)])
            pieces.append(sent)
        return pieces

    strips = strip_table(devices, spans).reshape(2 * spans * devices, devices, -1)

    def columns_pass(columns, place):
        mixed = mix("ugs,grsp->rup", strips, columns)
        half = spans * devices
        band = slice(starts[place], starts[place] + sizes[place])
        twiddle = tuple(jnp.tile(t[:, band].T, (1, spans))[:, :, None] for t in full_twiddle)
        turned = rotate((mixed[:, :half], mixed[:, half:]), twiddle)
        section_two = jnp.concatenate([part.astype(jnp.bfloat16) for part in turned], axis=0)
        section_two = section_two.reshape(-1, spans, devices, lead_len)
        return [
            mix("km,mjpc->kpjc", t[:, :, band].reshape(t.shape[0], -1), section_two)
            for t in group_tables
        ]

    count = len(sizes)
    totals, spread, gate = None, [], None
    queue = [fetch(0, None), fetch(1, None)]

    def gather_columns(place, totals):
        columns = spread[place]
        if totals is not None:
            columns, totals = lax.optimization_barrier((columns, totals))
        fresh = columns_pass(columns, place)
        if totals is None:
            return fresh
        return [old + new for old, new in zip(totals, fresh)]

    for place in range(count):
        got = queue.pop(0)
        if gate is not None:
            got = list(lax.optimization_barrier((*got, gate))[:-1])
        shares = rows_pass(jnp.stack(got), order, devices)
        if totals is not None:
            shares, totals = lax.optimization_barrier((shares, totals))
        gate = shares
        if place + AHEAD < count:
            queue.append(fetch(place + AHEAD, gate))
        spread.append(
            lax.all_to_all(shares, ("row", "col"), split_axis=0, concat_axis=0, tiled=True)
        )
        if place >= 1:
            totals = gather_columns(place - 1, totals)
    totals = gather_columns(count - 1, totals)
    pieces = [None] * len(tables)
    for group, total in zip(groups, totals):
        bands = total.astype(jnp.bfloat16).reshape(len(group), 2, steps * devices, col_width)
        for spot, place in enumerate(group):
            band_rows = lax.dynamic_slice_in_dim(bands[spot], heads[place], FS, 1)
            if distances[place] != 0:
                band_rows = shifted(band_rows, ("row", "col"), distances[place])
            pieces[place] = band_rows
    window = jnp.concatenate(pieces, axis=2)
    facet_tile = lax.dynamic_slice_in_dim(window, centre_col[my_index], FS, 2)
    taper_axis = 0.25 + 0.75 * jnp.sin(math.pi * (jnp.arange(FS, dtype=jnp.float32) + 0.5) / FS)
    weight = taper_axis[:, None] * taper_axis[None, :] * owned_count[my_index].astype(jnp.float32)
    return (facet_tile.astype(jnp.float32) * weight).astype(jnp.bfloat16)[None]


def solution(mesh):
    placed = (P(None, "row", "col"), P(), P(), P())
    return jax.shard_map(
        shards,
        mesh=mesh,
        in_specs=placed,
        out_specs=P(("row", "col"), None, None, None),
        check_vma=False,
    )
```

```python
import math

import jax
import jax.numpy as jnp
from jax import lax
from jax.sharding import PartitionSpec as P


N = 16384
FS = 1024
SPLIT = 128
PARTS = (1,) * 8
AHEAD = 2


def shifted(block, axis, distance):
    devices = range(lax.axis_size(axis))
    route = [((i - distance) % len(devices), i) for i in devices]
    return lax.ppermute(block, axis, route)


def dft_table(length):
    positions = jnp.arange(length, dtype=jnp.int32)
    turn_count = positions[:, None] * positions[None, :] % length
    angles = turn_count.astype(jnp.float32) * (-2.0 * math.pi / length)
    factor = 1.0 / math.sqrt(length)
    return (
        (jnp.cos(angles) * factor).astype(jnp.bfloat16),
        (jnp.sin(angles) * factor).astype(jnp.bfloat16),
    )


def twiddle_table(first_len, second_len, total):
    left_index = jnp.arange(first_len, dtype=jnp.int32)[:, None]
    right_index = jnp.arange(second_len, dtype=jnp.int32)[None, :]
    angles = (left_index * right_index % total).astype(jnp.float32) * (-2.0 * math.pi / total)
    return (jnp.cos(angles), jnp.sin(angles))


def paired_table(length):
    re_table, im_table = dft_table(length)
    return jnp.stack(
        (jnp.stack((re_table, -im_table), axis=1), jnp.stack((im_table, re_table), axis=1))
    )


def mix(formula, table, values):
    return jnp.einsum(formula, table, values, preferred_element_type=jnp.float32)


def rotate(pair, twiddle):
    return (
        pair[0] * twiddle[0] - pair[1] * twiddle[1],
        pair[0] * twiddle[1] + pair[1] * twiddle[0],
    )


def rows_pass(parts, order, devices):
    sources, _, row_count, width = parts.shape
    lead_len = N // SPLIT
    blocks = parts.reshape(sources, 2, row_count, width // SPLIT, SPLIT)
    blocks = blocks.transpose(2, 1, 0, 3, 4).reshape(row_count, 2 * lead_len, SPLIT)
    first = paired_table(lead_len).reshape(2 * lead_len, 2, sources, -1)
    first = jnp.take(first, order, axis=2).reshape(2 * lead_len, -1)
    mixed = mix("ka,rab->rkb", first, blocks)
    turned = rotate((mixed[:, :lead_len], mixed[:, lead_len:]), twiddle_table(lead_len, SPLIT, N))
    section_one = jnp.concatenate([part.astype(jnp.bfloat16) for part in turned], axis=2)
    table = paired_table(SPLIT).transpose(1, 0, 2, 3).reshape(2 * SPLIT, 2 * SPLIT)
    done = mix("kb,rpb->krp", table, section_one).astype(jnp.bfloat16)
    return done.reshape(devices, -1, row_count, lead_len).transpose(0, 2, 1, 3)


def strip_table(devices, spans):
    pairs = paired_table(devices)
    eye = jnp.eye(spans, dtype=jnp.bfloat16)
    full = pairs.transpose(0, 1, 3, 2)[:, :, None, :, None, :] * eye[None, None, :, None, :, None]
    return full.reshape(2 * spans * devices, devices, spans * 2)


def shards(sky_image, facet_rows, facet_offsets, facet_owner):
    row_devices = lax.axis_size("row")
    col_devices = lax.axis_size("col")
    devices = row_devices * col_devices
    strip_len = sky_image.shape[1] // col_devices
    sizes = [part * strip_len // sum(PARTS) for part in PARTS]
    starts = [sum(sizes[:place]) for place in range(len(sizes))]
    my_index = lax.axis_index(("row", "col"))
    device_ids = jnp.arange(devices, dtype=jnp.int32)
    matches = (facet_owner[None, :] == device_ids[:, None]).astype(jnp.int32)
    owned_count = jnp.sum(matches, axis=1)
    centre_row = jnp.where(owned_count > 0, jnp.sum(matches * facet_rows[None, :], axis=1), FS // 2)
    centre_col = jnp.sum(matches * facet_offsets[None, :], axis=1)

    lead_len = N // SPLIT
    spans = SPLIT // devices
    col_width = spans * lead_len
    reach_blocks = FS // (2 * col_width)
    distances = range(reach_blocks, -reach_blocks - 1, -1)
    steps = FS // devices + 1
    full_table = paired_table(strip_len).reshape(2, strip_len, 2, strip_len)
    tables, heads = [], []
    for distance in distances:
        start_row = centre_row[(my_index + distance) % devices] - FS // 2
        first_step = jnp.clip(start_row // devices, 0, strip_len - steps)
        tables.append(lax.dynamic_slice_in_dim(full_table, first_step, steps, 1))
        heads.append(start_row - first_step * devices)
    sides = [place for place, distance in enumerate(distances) if distance != 0]
    groups = [sides, [len(sides) // 2]]
    group_tables = [
        jnp.concatenate([tables[place] for place in group]).reshape(-1, 2, strip_len)
        for group in groups
    ]
    full_twiddle = twiddle_table(devices, strip_len, N)

    my_col = lax.axis_index("col")
    order = my_col ^ jnp.arange(col_devices, dtype=jnp.int32)
    image = sky_image.reshape(2, col_devices, strip_len, -1)

    def fetch(place, after):
        here = my_col
        if after is not None:
            here = lax.optimization_barrier((here, *after))[0]
        pieces, cut = [], []
        for hop in range(col_devices):
            sent = lax.dynamic_slice(
                image, (0, here ^ hop, starts[place], 0), (2, 1, sizes[place], image.shape[3])
            )[:, 0]
            cut.append(sent)
            if hop:
                sent = lax.ppermute(sent, "col", [(i, i ^ hop) for i in range(col_devices)])
            pieces.append(sent)
        return pieces, cut

    strips = strip_table(devices, spans).reshape(2 * spans * devices, devices, -1)

    def columns_pass(columns, place):
        mixed = mix("ugs,grsp->urp", strips, columns)
        half = spans * devices
        band = slice(starts[place], starts[place] + sizes[place])
        twiddle = tuple(jnp.repeat(t[:, band], spans, axis=0)[:, :, None] for t in full_twiddle)
        turned = rotate((mixed[:half], mixed[half:]), twiddle)
        section_two = jnp.concatenate([part.astype(jnp.bfloat16) for part in turned], axis=1)
        return [
            mix("km,zmc->kzc", t[:, :, band].reshape(t.shape[0], -1), section_two)
            for t in group_tables
        ]

    count = len(sizes)
    totals, spread, gate = None, [], None
    queue, cut = [], None
    for place in range(AHEAD):
        pieces, cut = fetch(place, cut)
        queue.append(pieces)

    def gather_columns(place, totals):
        columns = spread[place]
        if totals is not None:
            columns, totals = lax.optimization_barrier((columns, totals))
        fresh = columns_pass(columns, place)
        if totals is None:
            return fresh
        return [old + new for old, new in zip(totals, fresh)]

    for place in range(count):
        got = queue.pop(0)
        if gate is not None:
            got = list(lax.optimization_barrier((*got, gate))[:-1])
        shares = rows_pass(jnp.stack(got), order, devices)
        if totals is not None:
            shares, totals = lax.optimization_barrier((shares, totals))
        gate = shares
        if place + AHEAD < count:
            pieces, cut = fetch(place + AHEAD, (*cut, gate))
            queue.append(pieces)
        spread.append(
            lax.all_to_all(shares, ("row", "col"), split_axis=0, concat_axis=0, tiled=True)
        )
        if place >= 1:
            totals = gather_columns(place - 1, totals)
    totals = gather_columns(count - 1, totals)
    pieces = [None] * len(tables)
    for group, total in zip(groups, totals):
        bands = total.astype(jnp.bfloat16).reshape(len(group), 2, steps * devices, col_width)
        for spot, place in enumerate(group):
            band_rows = lax.dynamic_slice_in_dim(bands[spot], heads[place], FS, 1)
            if distances[place] != 0:
                band_rows = shifted(band_rows, ("row", "col"), distances[place])
            pieces[place] = band_rows
    window = jnp.concatenate(pieces, axis=2)
    facet_tile = lax.dynamic_slice_in_dim(window, centre_col[my_index], FS, 2)
    taper_axis = 0.25 + 0.75 * jnp.sin(math.pi * (jnp.arange(FS, dtype=jnp.float32) + 0.5) / FS)
    weight = taper_axis[:, None] * taper_axis[None, :] * owned_count[my_index].astype(jnp.float32)
    return (facet_tile.astype(jnp.float32) * weight).astype(jnp.bfloat16)[None]


def solution(mesh):
    placed = (P(None, "row", "col"), P(), P(), P())
    return jax.shard_map(
        shards,
        mesh=mesh,
        in_specs=placed,
        out_specs=P(("row", "col"), None, None, None),
        check_vma=False,
    )
```
